32 devices in a mesh: dp: 1 (over z), tp: 4 (over y), fsdp: 8 (over x, core).
Axes of the slice: x: 4, y: 4, z: 1, core: 2. Of those that a mesh axis runs over, the one named last changes fastest.
The devices are a block of a 4x4x8 slice.
Arguments:
- hidden: bfloat16 [8192, 4096], P(('dp', 'fsdp'))
- routes: int32 [2, 8192, 2], P(None, ('dp', 'fsdp'))
- norm_gain: bfloat16 [2, 4096], replicated
- router: bfloat16 [2, 4096, 16], replicated
- w_gate: bfloat16 [2, 16, 4096, 960], P(None, None, 'fsdp', 'tp')
- w_up: bfloat16 [2, 16, 4096, 960], P(None, None, 'fsdp', 'tp')
- w_down: bfloat16 [2, 16, 960, 4096], P(None, None, 'tp', 'fsdp')
Outputs:
- output: bfloat16 [8192, 4096], P(('dp', 'fsdp'))
All inputs are finite; a program needn't handle non-finite values.
Results may differ from the reference program's by a relative error of at most 0.0165296.
Values are sent between devices in bfloat16 or wider.
A program may use at most 768 MiB of HBM per device.

```python
import jax
import jax.numpy as jnp
from jax import lax

D_MODEL = 4096
D_FF = 960
EXPERTS = 16
TOP_K = 2
LAYERS = 2
TOK_DEV = 1024
TOKENS = 8192
TILE_ROWS = 128
NUM_TILES = (TOP_K * TOKENS + TILE_ROWS - 1) // TILE_ROWS + EXPERTS
NORM_EPS = 1e-5


def draw_routes(key):
    key_first, key_second, key_offset = jax.random.split(key, 3)
    pick_a = jax.random.randint(key_first, (LAYERS, TOKENS), 0, EXPERTS)
    pick_b = jax.random.randint(key_second, (LAYERS, TOKENS), 0, EXPERTS)
    slot_pos = jnp.broadcast_to(jnp.arange(TOKENS) % TOK_DEV, (LAYERS, TOKENS))
    first_pick = jnp.where(slot_pos < EXPERTS, slot_pos, jnp.minimum(pick_a, pick_b))
    offset_pick = jax.random.randint(key_offset, (LAYERS, TOKENS), 1, EXPERTS)
    second_pick = (first_pick + offset_pick) % EXPERTS
    return jnp.stack([first_pick, second_pick], axis=-1).astype(jnp.int32)


def setup_inputs(seed: int = 0, part: int = 0) -> dict:
    root_key = jax.random.key(seed)
    shared_key, part_root = jax.random.split(root_key)
    part_key = jax.random.fold_in(part_root, part)
    key_hidden, key_route = jax.random.split(part_key)
    key_gain, key_router, key_gate, key_up, key_down = jax.random.split(shared_key, 5)
    hidden = jax.random.normal(key_hidden, (TOKENS, D_MODEL), jnp.float32).astype(jnp.bfloat16)
    routes = draw_routes(key_route)
    norm_gain = (1.0 + 0.5 * jax.random.normal(key_gain, (LAYERS, D_MODEL), jnp.float32)).astype(jnp.bfloat16)
    router = (jax.random.normal(key_router, (LAYERS, D_MODEL, EXPERTS), jnp.float32) * D_MODEL ** -0.5).astype(jnp.bfloat16)
    w_gate = (jax.random.normal(key_gate, (LAYERS, EXPERTS, D_MODEL, D_FF), jnp.float32) * D_MODEL ** -0.5).astype(jnp.bfloat16)
    w_up = (jax.random.normal(key_up, (LAYERS, EXPERTS, D_MODEL, D_FF), jnp.float32) * D_MODEL ** -0.5).astype(jnp.bfloat16)
    w_down = (jax.random.normal(key_down, (LAYERS, EXPERTS, D_FF, D_MODEL), jnp.float32) * (2.0 * D_FF ** -0.5)).astype(jnp.bfloat16)
    return {'hidden': hidden, 'routes': routes, 'norm_gain': norm_gain, 'router': router, 'w_gate': w_gate, 'w_up': w_up, 'w_down': w_down}


def moe_layer(hidden, routes, norm_gain, router, w_gate, w_up, w_down):
    hidden_f = hidden.astype(jnp.float32)
    inv_rms = lax.rsqrt(jnp.mean(hidden_f * hidden_f, axis=-1, keepdims=True) + NORM_EPS)
    normed = (hidden_f * inv_rms * norm_gain.astype(jnp.float32)).astype(jnp.bfloat16)
    logits = jnp.dot(normed, router, preferred_element_type=jnp.float32)
    onehot = (routes[:, :, None] == jnp.arange(EXPERTS)[None, None, :]).astype(jnp.float32)
    picked = jnp.sum(onehot * logits[:, None, :], axis=-1)
    gate_probs = jax.nn.softmax(picked, axis=-1)
    flat_ids = routes.reshape(-1)
    sort_order = jnp.argsort(flat_ids, stable=True)
    sorted_ids = flat_ids[sort_order]
    counts = jnp.bincount(flat_ids, length=EXPERTS)
    padded = (counts + TILE_ROWS - 1) // TILE_ROWS * TILE_ROWS
    pad_end = jnp.cumsum(padded)
    pad_start = pad_end - padded
    group_start = jnp.cumsum(counts) - counts
    target_slot = pad_start[sorted_ids] + jnp.arange(TOP_K * TOKENS) - group_start[sorted_ids]
    tile_start = jnp.arange(NUM_TILES) * TILE_ROWS
    tile_expert = jnp.minimum(jnp.sum((pad_end[None, :] <= tile_start[:, None]).astype(jnp.int32), axis=1), EXPERTS - 1)
    packed = jnp.zeros((NUM_TILES * TILE_ROWS, D_MODEL), jnp.bfloat16).at[target_slot].set(normed[sort_order // TOP_K])

    def tile_body(tile_args):
        tile_rows, expert_id = tile_args
        gate_out = jnp.dot(tile_rows, w_gate[expert_id], preferred_element_type=jnp.float32)
        up_out = jnp.dot(tile_rows, w_up[expert_id], preferred_element_type=jnp.float32)
        act_rows = (jax.nn.silu(gate_out) * up_out).astype(jnp.bfloat16)
        return jnp.dot(act_rows, w_down[expert_id], preferred_element_type=jnp.float32)

    tile_out = lax.map(tile_body, (packed.reshape(NUM_TILES, TILE_ROWS, D_MODEL), tile_expert))
    tile_out = tile_out.reshape(NUM_TILES * TILE_ROWS, D_MODEL)
    slot_of = jnp.zeros((TOP_K * TOKENS,), jnp.int32).at[sort_order].set(target_slot)
    expert_out = tile_out[slot_of].reshape(TOKENS, TOP_K, D_MODEL)
    mixed_out = jnp.sum(gate_probs[:, :, None] * expert_out, axis=1)
    return (hidden_f + mixed_out).astype(jnp.bfloat16)


def reference(hidden, routes, norm_gain, router, w_gate, w_up, w_down):
    def layer_step(state_in, layer_args):
        layer_routes, layer_gain, layer_router, layer_gate, layer_up, layer_down = layer_args
        return moe_layer(state_in, layer_routes, layer_gain, layer_router, layer_gate, layer_up, layer_down), None

    final_hidden, unused_ys = lax.scan(layer_step, hidden, (routes, norm_gain, router, w_gate, w_up, w_down))
    return final_hidden
```

```python
import jax
import jax.numpy as jnp
from jax import lax
from jax.experimental import pallas as pl
from jax.experimental.pallas import tpu as pltpu
from jax.sharding import PartitionSpec as P

NORM_EPS = 1e-5
CHUNKS = 4
CORES = 2
VMEM_BYTES = 56 * 1024 * 1024
MESH = pl.DeviceIdType.MESH


def wide(ids, width):
    return jnp.concatenate([ids] * (width // ids.shape[1]), axis=1)


class Send:
    def __init__(self, kind, axis, size, src, dst_shape, piece, src_at, dst_at):
        self.kind, self.axis, self.size = kind, axis, size
        self.src, self.dst = src, jax.ShapeDtypeStruct(dst_shape, src.dtype)
        self.piece, self.src_at, self.dst_at = piece, src_at, dst_at

    def scratch(self):
        dma = pltpu.SemaphoreType.DMA
        return [pltpu.VMEM(self.piece, self.src.dtype), dma((self.size - 1,)), dma((self.size - 1,)), dma((2,))]

    def place(self):
        me = lax.axis_index(self.axis)
        return me // CORES if self.axis == 'fsdp' else me

    def device(self, peer):
        if self.axis == 'fsdp':
            return {'fsdp': peer * CORES + lax.rem(lax.axis_index('fsdp'), CORES)}
        return {self.axis: peer}

    def peers(self):
        me = self.place()
        return [lax.rem(me + dist, self.size) for dist in range(1, self.size)]

    def remote(self, refs):
        src, dst, _, send_sem, recv_sem, _ = refs
        me = self.place()
        return [pltpu.make_async_remote_copy(src_ref=self.src_at(src, peer), dst_ref=self.dst_at(dst, me), send_sem=send_sem.at[num], recv_sem=recv_sem.at[num], device_id=self.device(peer), device_id_type=MESH) for num, peer in enumerate(self.peers())]

    def take(self, refs):
        return pltpu.make_async_copy(self.src_at(refs[0], self.place()), refs[2], refs[5].at[0])

    def put(self, refs):
        return pltpu.make_async_copy(refs[2], self.dst_at(refs[1], self.place()), refs[5].at[1])


IDS = {}


def carry(name, body, grid, inputs, in_specs, outputs, out_specs, scratch, sends, flops, item=0):
    num_in, num_out, num_scr, num_send = len(inputs), len(outputs), len(scratch), len(sends)
    any_spec = pl.BlockSpec(memory_space=pl.ANY)

    def kernel(*refs):
        ins, refs = refs[:num_in], refs[num_in:]
        srcs, refs = refs[:num_send], refs[num_send:]
        outs, refs = refs[:num_out], refs[num_out:]
        dsts, refs = refs[:num_send], refs[num_send:]
        scr, refs = refs[:num_scr], refs[num_scr:]
        groups = [(srcs[num], dsts[num]) + tuple(refs[4 * num:4 * num + 4]) for num in range(num_send)]
        step = pl.program_id(0)
        if sends:
            @pl.when(step == 0)
            def _():
                barrier = pltpu.get_barrier_semaphore()
                greeted = 0
                for send in {send.axis: send for send in sends}.values():
                    for peer in send.peers():
                        pl.semaphore_signal(barrier, inc=1, device_id=send.device(peer), device_id_type=MESH)
                        greeted += 1
                pl.semaphore_wait(barrier, greeted)
                for send, group in zip(sends, groups):
                    for copy in send.remote(group):
                        copy.start()
                for send, group in zip(sends, groups):
                    send.take(group).start()
                for send, group in zip(sends, groups):
                    send.take(group).wait()
                    send.put(group).start()
        if body is not None:
            body(*ins, *outs, *scr)
        if sends:
            @pl.when(step == grid - 1)
            def _():
                for send, group in zip(sends, groups):
                    send.put(group).wait()
                    for copy in send.remote(group):
                        copy.wait()

    params = dict(vmem_limit_bytes=VMEM_BYTES, dimension_semantics=("arbitrary",))
    if sends:
        key = (name, item) + tuple(send.kind for send in sends)
        params.update(collective_id=IDS.setdefault(key, len(IDS)), has_side_effects=True)
    results = pl.pallas_call(
        kernel,
        grid=(grid,),
        in_specs=in_specs + [any_spec] * num_send,
        out_specs=out_specs + [any_spec] * num_send,
        out_shape=outputs + [send.dst for send in sends],
        scratch_shapes=scratch + [item for send in sends for item in send.scratch()],
        compiler_params=pltpu.CompilerParams(**params),
        cost_estimate=pl.CostEstimate(flops=flops, bytes_accessed=1 << 22, transcendentals=0),
        name="_".join([name] + [send.kind for send in sends]),
    )(*inputs, *[send.src for send in sends])
    return results[:num_out], results[num_out:]


CONTRACT_LAST = (((1,), (1,)), ((), ()))


def up_call(layer, item, h, ids, router_pad, weights, sends):
    rows, depth = h.shape
    _, experts, ff, half = weights[0].shape
    pad = router_pad.shape[1]
    tile = min(rows, 512)

    def body(h_ref, ids_ref, router_ref, gate_own, gate_peer, up_own, up_peer, out_ref):
        expert = pl.program_id(0)
        core = lax.rem(lax.axis_index('fsdp'), CORES)
        own = pl.ds(pl.multiple_of(core * half, half), half)
        peer = pl.ds(pl.multiple_of((1 - core) * half, half), half)

        @pl.when(expert == 0)
        def _():
            for start in range(0, rows, tile):
                sl = slice(start, start + tile)
                out_ref[sl, 0:pad] = jnp.dot(h_ref[sl, :], router_ref[...], preferred_element_type=jnp.float32)
                out_ref[sl, pad:4 * pad] = jnp.zeros((tile, 3 * pad), jnp.float32)

        for start in range(0, rows, tile):
            sl = slice(start, start + tile)
            is_a = wide(ids_ref[0, 0, sl, :], pad)[:, :ff] == expert
            is_b = wide(ids_ref[0, 1, sl, :], pad)[:, :ff] == expert
            for num, (w_own, w_peer) in enumerate(((gate_own, gate_peer), (up_own, up_peer))):
                both = jnp.concatenate([w_own[0, 0], w_peer[0, 0]], axis=1)
                prod = lax.dot_general(jnp.concatenate([h_ref[sl, own], h_ref[sl, peer]], axis=1), both, CONTRACT_LAST, preferred_element_type=jnp.float32)
                col_a, col_b = num * pad, (2 + num) * pad
                out_ref[sl, col_a:col_a + ff] = jnp.where(is_a, prod, out_ref[sl, col_a:col_a + ff])
                out_ref[sl, col_b:col_b + ff] = jnp.where(is_b, prod, out_ref[sl, col_b:col_b + ff])

    whole = lambda shape: pl.BlockSpec(shape, lambda e: (0, 0))
    weight = pl.BlockSpec((1, 1, ff, half), lambda e: (layer, e, 0, 0))
    outs, got = carry(
        "up", body, experts, [h, ids, router_pad, *weights],
        [whole((rows, depth)), pl.BlockSpec((1, 2, rows, 128), lambda e: (item, 0, 0, 0)), whole((depth, pad))] + [weight] * 4,
        [jax.ShapeDtypeStruct((rows, 4 * pad), jnp.float32)], [whole((rows, 4 * pad))], [], sends,
        rows * depth * 2 * pad * experts * 2, item)
    return outs[0], got


def act_kernel(ff, pad, uv_ref, a_ref, b_ref, out_ref):
    lane = lax.broadcasted_iota(jnp.int32, (uv_ref.shape[0], pad), 1)
    gate_a = uv_ref[:, 0:pad]
    pick = lambda ids: jnp.sum(jnp.where(lane == wide(ids, pad) + ff, gate_a, 0.0), axis=1, keepdims=True)
    log_a, log_b = pick(a_ref[...]), pick(b_ref[...])
    top = jnp.maximum(log_a, log_b)
    exp_a, exp_b = jnp.exp(log_a - top), jnp.exp(log_b - top)
    total = exp_a + exp_b

    def parts(prob):
        high = prob.astype(jnp.bfloat16).astype(jnp.float32)
        mid = (prob - high).astype(jnp.bfloat16).astype(jnp.float32)
        return high, mid, prob - high - mid

    def swiglu(gate, up):
        return gate * jax.nn.sigmoid(gate) * up

    def assemble(act, prob):
        blk = jnp.where(lane < ff, act, 0.0)
        for num, part in enumerate(parts(prob)):
            blk = jnp.where(lane == ff + num, part, blk)
        return blk.astype(jnp.bfloat16)

    out_ref[:, 0:pad] = assemble(swiglu(gate_a, uv_ref[:, pad:2 * pad]), exp_a / total)
    out_ref[:, pad:2 * pad] = assemble(swiglu(uv_ref[:, 2 * pad:3 * pad], uv_ref[:, 3 * pad:4 * pad]), exp_b / total)


def act_call(uv, ids_a, ids_b, ff, pad):
    rows = uv.shape[0]
    return pl.pallas_call(
        lambda *refs: act_kernel(ff, pad, *refs),
        out_shape=jax.ShapeDtypeStruct((rows, 2 * pad), jnp.bfloat16),
        compiler_params=pltpu.CompilerParams(vmem_limit_bytes=16 * 1024 * 1024),
        cost_estimate=pl.CostEstimate(flops=rows * pad * 600, bytes_accessed=rows * pad * 20, transcendentals=rows * pad * 2),
        name="swiglu_and_weights",
    )(uv, ids_a, ids_b)


def down_call(layer, item, m_all, ids, weights, pad, owners, quarters, sends):
    rows = m_all.shape[0]
    _, experts, ff, half = weights[0].shape
    cols = CORES * half
    tile = min(rows, 512)

    def body(m_ref, ids_ref, down_own, down_peer, out_ref, acc_ref, wide_ref, prob_ref):
        expert = pl.program_id(0)
        me_core = lax.rem(lax.axis_index('fsdp'), CORES)

        @pl.when(expert == 0)
        def _():
            for start in range(0, rows, tile):
                sl = slice(start, start + tile)
                lane = lax.broadcasted_iota(jnp.int32, (tile, pad), 1)
                is_prob = (lane >= ff) & (lane < ff + 3)
                for num in range(2):
                    blk = m_ref[sl, num * pad:(num + 1) * pad].astype(jnp.float32)
                    wide_ref[sl, num * pad:(num + 1) * pad] = blk
                    prob = jnp.sum(jnp.where(is_prob, blk, 0.0), axis=1, keepdims=True)
                    prob_ref[sl, num * 128:(num + 1) * 128] = jnp.broadcast_to(prob, (tile, 128))
                acc_ref[sl, :] = jnp.zeros((tile, cols), jnp.float32)

        for start in range(0, rows, tile):
            sl = slice(start, start + tile)
            ids_a, ids_b = ids_ref[0, 0, sl, :], ids_ref[0, 1, sl, :]
            is_a, is_b = wide(ids_a, pad)[:, :ff] == expert, wide(ids_b, pad)[:, :ff] == expert
            act = jnp.where(is_a, wide_ref[sl, 0:ff], jnp.where(is_b, wide_ref[sl, pad:pad + ff], 0.0)).astype(jnp.bfloat16)
            prob = jnp.where(ids_a == expert, prob_ref[sl, 0:128], jnp.where(ids_b == expert, prob_ref[sl, 128:256], 0.0))
            for core, w_ref in ((me_core, down_own), (1 - me_core, down_peer)):
                prod = jnp.dot(act, w_ref[0, 0], preferred_element_type=jnp.float32)
                acc_ref[sl, pl.ds(pl.multiple_of(core * half, half), half)] += wide(prob, half) * prod

        @pl.when(expert == experts - 1)
        def _():
            per = rows // owners
            sub = per // quarters
            for owner in range(owners):
                for quarter in range(quarters):
                    start = owner * per + quarter * sub
                    out_ref[quarter, owner * sub:(owner + 1) * sub, :] = acc_ref[start:start + sub, :].astype(jnp.bfloat16)

    whole = lambda shape: pl.BlockSpec(shape, lambda e: (0,) * len(shape))
    weight = pl.BlockSpec((1, 1, ff, half), lambda e: (layer, e, 0, 0))
    out_shape = (quarters, rows // quarters, cols)
    outs, got = carry(
        "down", body, experts, [m_all, ids, *weights],
        [whole((rows, 2 * pad)), pl.BlockSpec((1, 2, rows, 128), lambda e: (item, 0, 0, 0)), weight, weight],
        [jax.ShapeDtypeStruct(out_shape, jnp.bfloat16)], [whole(out_shape)],
        [pltpu.VMEM((rows, cols), jnp.float32), pltpu.VMEM((rows, 2 * pad), jnp.float32), pltpu.VMEM((rows, 256), jnp.float32)], sends,
        rows * pad * cols * experts * 2, item)
    return outs[0], got


def send_only(sends):
    return carry("move", None, 1, [], [], [], [], [], sends, 1 << 30)[1]


def solution(mesh):
    tok_axes = ('dp', 'fsdp')
    quarters = mesh.shape['tp']
    owners = mesh.shape['fsdp'] // CORES
    lines = [[chip * CORES + core for chip in range(owners)] for core in range(CORES)]
    swap = [(src, src // CORES * CORES + (src + 1) % CORES) for src in range(mesh.shape['fsdp'])]

    def exchange_x(part):
        blocks = jnp.broadcast_to(part[None], (owners,) + part.shape)
        return lax.all_to_all(blocks, 'fsdp', split_axis=0, concat_axis=0, tiled=True, axis_index_groups=lines)

    def local_step(hidden, routes, norm_gain, router, w_gate, w_up, w_down):
        layers, num_tokens, _ = routes.shape
        dim = hidden.shape[1]
        half, ff, experts = w_gate.shape[2], w_gate.shape[3], w_gate.shape[1]
        block = half * CORES
        pad = -(-(ff + experts) // 128) * 128
        per = num_tokens // CHUNKS
        sub = per // quarters
        me_chip, me_t = lax.axis_index('fsdp') // CORES, lax.axis_index('tp')
        total = layers * CHUNKS

        def tokens(item):
            return slice(item % CHUNKS * per, (item % CHUNKS + 1) * per)

        def lanes(ids):
            return jnp.broadcast_to(ids.reshape(-1)[:, None], (ids.size, 128))

        def send_input(chunk):
            rows = pl.ds(chunk * per, per)
            return Send("x%d" % chunk, 'fsdp', owners, hidden, (owners, per, block), (per, block),
                        lambda ref, peer: ref.at[rows, pl.ds(pl.multiple_of(peer * block, block), block)], lambda ref, me: ref.at[me])

        def send_part(chunk):
            return Send("part%d" % chunk, 'fsdp', owners, hidden, (owners, sub, block), (sub, block),
                        lambda ref, peer: ref.at[pl.ds(pl.multiple_of(chunk * per + lax.axis_index('tp') * sub, sub), sub), pl.ds(pl.multiple_of(peer * block, block), block)], lambda ref, me: ref.at[me])

        def send_act(act):
            return Send("act", 'fsdp', owners, act, (owners,) + act.shape, act.shape, lambda ref, peer: ref, lambda ref, me: ref.at[me])

        def send_sum(y):
            return Send("sum", 'tp', quarters, y, y.shape, y.shape[1:], lambda ref, peer: ref.at[peer], lambda ref, me: ref.at[me])

        def send_h(h):
            return Send("h", 'tp', quarters, h, (owners, quarters) + h.shape[1:], h.shape, lambda ref, peer: ref, lambda ref, me: ref.at[:, me])

        def send_rows(x):
            return Send("rows", 'fsdp', owners, x, (sub, dim), (sub, block), lambda ref, peer: ref.at[peer],
                        lambda ref, me: ref.at[:, pl.ds(pl.multiple_of(me * block, block), block)])

        def send_out(x):
            return Send("out", 'tp', quarters, x, (quarters,) + x.shape, x.shape, lambda ref, peer: ref, lambda ref, me: ref.at[me])

        hidden_f = hidden.astype(jnp.float32)
        inv_own = lax.rsqrt(jnp.mean(hidden_f * hidden_f, axis=-1) + NORM_EPS)
        facts = jnp.concatenate([inv_own[None], routes.transpose(0, 2, 1).reshape(-1, num_tokens).astype(jnp.float32)], axis=0)
        facts = exchange_x(facts)
        inv_all = facts[:, 0]
        all_routes = facts[:, 1:].astype(jnp.int32).reshape(owners, layers, 2, num_tokens)

        def pair(weight):
            return weight, lax.ppermute(weight, 'fsdp', swap)

        up_weights = pair(w_gate.swapaxes(2, 3)) + pair(w_up.swapaxes(2, 3))
        down_weights = pair(w_down)
        gains = lax.dynamic_slice_in_dim(norm_gain, me_chip * block, block, 1).astype(jnp.float32)
        my_router = lax.dynamic_slice_in_dim(router, me_chip * block, block, 1)
        router_pad = jnp.pad(my_router, ((0, 0), (0, 0), (ff, pad - ff - experts)))
        ids = all_routes.reshape(owners, layers, 2, CHUNKS, per).transpose(1, 3, 2, 0, 4).reshape(total, 2, owners * per, 1)
        ids = jnp.broadcast_to(ids, ids.shape[:3] + (128,))
        own = [[lanes(routes[item // CHUNKS, tokens(item), num]) for num in range(2)] for item in range(total)]

        h, x_quarter, uv, act, m_all, y, ready, rows, out = {}, {}, {}, {}, {}, {}, {}, {}, {}

        def arrive_input(chunk, x_all):
            x_f = x_all.astype(jnp.float32)
            h[chunk] = (x_f * inv_all[:, tokens(chunk), None] * gains[0]).astype(jnp.bfloat16).reshape(owners * per, block)
            x_quarter[chunk] = lax.dynamic_slice_in_dim(x_all, me_t * sub, sub, 1)

        def arrive_part(chunk, got):
            x_quarter[chunk] = got
            inv = lax.dynamic_slice_in_dim(inv_all, chunk * per + me_t * sub, sub, 1)
            ready[chunk - CHUNKS] = (got.astype(jnp.float32) * inv[:, :, None] * gains[0]).astype(jnp.bfloat16)

        def arrive_act(item, got):
            m_all[item] = got.reshape(owners * per, 2 * pad)

        def arrive_sum(item, got):
            summed = jnp.sum(got.astype(jnp.float32), axis=0).reshape(owners, sub, block)
            x_new = (x_quarter[item].astype(jnp.float32) + summed).astype(jnp.bfloat16)
            ready[item] = x_new
            if item + CHUNKS < total:
                x_f = x_new.astype(jnp.float32)
                squares = jnp.sum(exchange_x(jnp.sum(x_f * x_f, axis=-1)), axis=0)
                inv = lax.rsqrt(squares / dim + NORM_EPS)
                x_quarter[item + CHUNKS] = x_new
                ready[item] = (x_f * inv[:, :, None] * gains[item // CHUNKS + 1]).astype(jnp.bfloat16)

        def arrive_h(item, got):
            h[item + CHUNKS] = got.reshape(owners * per, block)

        def arrive_rows(item, got):
            rows[item] = got

        def arrive_out(item, got):
            out[item] = got.reshape(per, dim)

        def inner(item):
            return item + CHUNKS < total

        first = [send_input(0)] + [send_part(chunk) for chunk in range(1, 2)]
        got = send_only(first)
        arrive_input(0, got[0])
        arrive_part(1, got[1])
        for step in range(total + 4):
            work = []
            if step == 0:
                for chunk in range(2, CHUNKS):
                    work.append((send_part(chunk), arrive_part, chunk))
            if step + 1 < CHUNKS:
                work.append((send_h(ready[step + 1 - CHUNKS]), arrive_h, step + 1 - CHUNKS))
            if 0 <= step - 2 < total:
                item = step - 2
                uv_own = lax.psum_scatter(uv[item], 'fsdp', scatter_dimension=0, tiled=True, axis_index_groups=lines)
                act[item] = act_call(uv_own, own[item][0], own[item][1], ff, pad)
                work.append((send_act(act[item]), arrive_act, item))
            if 0 <= step - 3 < total:
                work.append((send_sum(y[step - 3]), arrive_sum, step - 3))
            sends = [entry[0] for entry in work]
            if step < total:
                uv[step], got = up_call(step // CHUNKS, step, h[step], ids, router_pad[step // CHUNKS], up_weights, sends)
            else:
                got = send_only(sends) if sends else []
            for (_, arrive, item), value in zip(work, got):
                arrive(item, value)
            work = []
            if 0 <= step - 4 < total and not inner(step - 4):
                work.append((send_out(rows[step - 4]), arrive_out, step - 4))
            if 0 <= step - 3 < total:
                if inner(step - 3):
                    work.append((send_h(ready[step - 3]), arrive_h, step - 3))
                else:
                    work.append((send_rows(ready[step - 3]), arrive_rows, step - 3))
            sends = [entry[0] for entry in work]
            got = []
            if 0 <= step - 2 < total:
                item = step - 2
                y[item], got = down_call(item // CHUNKS, item, m_all[item], ids, down_weights, pad, owners, quarters, sends)
            elif sends:
                got = send_only(sends)
            for (_, arrive, item), value in zip(work, got):
                arrive(item, value)
        return jnp.concatenate([out[item] for item in range(total - CHUNKS, total)], axis=0)

    weight_in = P(None, None, 'fsdp', 'tp')
    weight_out = P(None, None, 'tp', 'fsdp')
    return jax.shard_map(local_step, mesh=mesh, in_specs=(P(tok_axes, None), P(None, tok_axes, None), P(None, None), P(None, None, None), weight_in, weight_in, weight_out), out_specs=P(tok_axes, None), check_vma=False)
```

```python
import jax
import jax.numpy as jnp
from jax import lax
from jax.experimental import pallas as pl
from jax.experimental.pallas import tpu as pltpu
from jax.sharding import PartitionSpec as P

NORM_EPS = 1e-5
CHUNKS = 4
UP_EXPERTS = 2
DOWN_EXPERTS = 2
CORES = 2
VMEM_BYTES = 56 * 1024 * 1024
MESH = pl.DeviceIdType.MESH


def wide(ids, width):
    return jnp.concatenate([ids] * (width // ids.shape[1]), axis=1)


class Send:
    def __init__(self, kind, axis, size, src, dst_shape, piece, src_at, dst_at, half_at=None):
        self.half_at = half_at if size == 4 else None
        self.kind, self.axis, self.size = kind, axis, size
        self.src, self.dst = src, jax.ShapeDtypeStruct(dst_shape, src.dtype)
        self.piece, self.src_at, self.dst_at = piece, src_at, dst_at

    def scratch(self):
        dma = pltpu.SemaphoreType.DMA
        return [pltpu.VMEM(self.piece, self.src.dtype), dma((self.size,)), dma((self.size,)), dma((2,))]

    def place(self):
        me = lax.axis_index(self.axis)
        return me // CORES if self.axis == 'fsdp' else me

    def device(self, peer):
        if self.axis == 'fsdp':
            return {'fsdp': peer * CORES + lax.rem(lax.axis_index('fsdp'), CORES)}
        return {self.axis: peer}

    def peers(self):
        me = self.place()
        dists = range(1, self.size)
        if self.half_at is not None:
            dists = (1, self.size - 1)
        return [lax.rem(me + dist, self.size) for dist in dists]

    def relay(self, refs):
        dst, send_sem, recv_sem = refs[1], refs[3], refs[4]
        after, before = self.peers()
        return [pltpu.make_async_remote_copy(src_ref=self.half_at(dst, origin, num), dst_ref=self.half_at(dst, origin, num), send_sem=send_sem.at[2 + num], recv_sem=recv_sem.at[2 + num], device_id=self.device(peer), device_id_type=MESH) for num, (origin, peer) in enumerate(((before, after), (after, before)))]

    def remote(self, refs):
        src, dst, _, send_sem, recv_sem, _ = refs
        me = self.place()
        return [pltpu.make_async_remote_copy(src_ref=self.src_at(src, peer), dst_ref=self.dst_at(dst, me), send_sem=send_sem.at[num], recv_sem=recv_sem.at[num], device_id=self.device(peer), device_id_type=MESH) for num, peer in enumerate(self.peers())]

    def take(self, refs):
        return pltpu.make_async_copy(self.src_at(refs[0], self.place()), refs[2], refs[5].at[0])

    def put(self, refs):
        return pltpu.make_async_copy(refs[2], self.dst_at(refs[1], self.place()), refs[5].at[1])


IDS = {}


def carry(name, body, grid, inputs, in_specs, outputs, out_specs, scratch, sends, flops, item=0):
    num_in, num_out, num_scr, num_send = len(inputs), len(outputs), len(scratch), len(sends)
    any_spec = pl.BlockSpec(memory_space=pl.ANY)

    def kernel(*refs):
        ins, refs = refs[:num_in], refs[num_in:]
        srcs, refs = refs[:num_send], refs[num_send:]
        outs, refs = refs[:num_out], refs[num_out:]
        dsts, refs = refs[:num_send], refs[num_send:]
        scr, refs = refs[:num_scr], refs[num_scr:]
        groups = [(srcs[num], dsts[num]) + tuple(refs[4 * num:4 * num + 4]) for num in range(num_send)]
        step = pl.program_id(0)
        if sends:
            @pl.when(step == 0)
            def _():
                barrier = pltpu.get_barrier_semaphore()
                greeted = 0
                for send in {send.axis: send for send in sorted(sends, key=lambda send: send.half_at is None)}.values():
                    for peer in send.peers():
                        pl.semaphore_signal(barrier, inc=1, device_id=send.device(peer), device_id_type=MESH)
                        greeted += 1
                pl.semaphore_wait(barrier, greeted)
                for send, group in zip(sends, groups):
                    for copy in send.remote(group):
                        copy.start()
                for send, group in zip(sends, groups):
                    send.take(group).start()
                for send, group in zip(sends, groups):
                    send.take(group).wait()
                    send.put(group).start()
        if body is not None:
            body(*ins, *outs, *scr)
        relays = [(send, group) for send, group in zip(sends, groups) if send.half_at is not None]
        if relays:
            @pl.when(step == (grid - 1) * 5 // 8)
            def _():
                for send, group in relays:
                    for copy in send.remote(group):
                        copy.wait_recv()
                    for copy in send.relay(group):
                        copy.start()
        if sends:
            @pl.when(step == grid - 1)
            def _():
                for send, group in zip(sends, groups):
                    send.put(group).wait()
                    for copy in send.remote(group):
                        copy.wait() if send.half_at is None else copy.wait_send()
                    if send.half_at is not None:
                        for copy in send.relay(group):
                            copy.wait()

    params = dict(vmem_limit_bytes=VMEM_BYTES, dimension_semantics=("arbitrary",))
    if sends:
        key = (name, item) + tuple(send.kind for send in sends)
        params.update(collective_id=IDS.setdefault(key, len(IDS)), has_side_effects=True)
    results = pl.pallas_call(
        kernel,
        grid=(grid,),
        in_specs=in_specs + [any_spec] * num_send,
        out_specs=out_specs + [any_spec] * num_send,
        out_shape=outputs + [send.dst for send in sends],
        scratch_shapes=scratch + [item for send in sends for item in send.scratch()],
        compiler_params=pltpu.CompilerParams(**params),
        cost_estimate=pl.CostEstimate(flops=flops, bytes_accessed=1 << 22, transcendentals=0),
        name="_".join([name] + [send.kind for send in sends]),
    )(*inputs, *[send.src for send in sends])
    return results[:num_out], results[num_out:]


CONTRACT_LAST = (((1,), (1,)), ((), ()))


def up_call(layer, item, h, ids, router_pad, weights, sends):
    rows, depth = h.shape
    _, experts, ff, half = weights[0].shape
    pad = router_pad.shape[1]
    tile = min(rows, 512)

    def body(h_ref, ids_ref, router_ref, gate_own, gate_peer, up_own, up_peer, out_ref):
        expert = pl.program_id(0)
        core = lax.rem(lax.axis_index('fsdp'), CORES)
        own = pl.ds(pl.multiple_of(core * half, half), half)
        peer = pl.ds(pl.multiple_of((1 - core) * half, half), half)

        @pl.when(expert == 0)
        def _():
            @pl.loop(0, rows, step=256)
            def _(start):
                sl = pl.ds(pl.multiple_of(start, 256), 256)
                out_ref[sl, 0:pad] = jnp.dot(h_ref[sl, :], router_ref[...], preferred_element_type=jnp.float32)
                out_ref[sl, pad:4 * pad] = jnp.zeros((256, 3 * pad), jnp.float32)

        for turn, start in [(turn, start) for turn in range(UP_EXPERTS) for start in range(0, rows, tile)]:
            sl = slice(start, start + tile)
            expert = pl.program_id(0) * UP_EXPERTS + turn
            is_a = wide(ids_ref[0, 0, sl, :], pad)[:, :ff] == expert
            is_b = wide(ids_ref[0, 1, sl, :], pad)[:, :ff] == expert
            for num, (w_own, w_peer) in enumerate(((gate_own, gate_peer), (up_own, up_peer))):
                both = jnp.concatenate([w_own[0, turn], w_peer[0, turn]], axis=1)
                prod = lax.dot_general(jnp.concatenate([h_ref[sl, own], h_ref[sl, peer]], axis=1), both, CONTRACT_LAST, preferred_element_type=jnp.float32)
                col_a, col_b = num * pad, (2 + num) * pad
                out_ref[sl, col_a:col_a + ff] = jnp.where(is_a, prod, out_ref[sl, col_a:col_a + ff])
                out_ref[sl, col_b:col_b + ff] = jnp.where(is_b, prod, out_ref[sl, col_b:col_b + ff])

    whole = lambda shape: pl.BlockSpec(shape, lambda e: (0, 0))
    weight = pl.BlockSpec((1, UP_EXPERTS, ff, half), lambda e: (layer, e, 0, 0))
    outs, got = carry(
        "up", body, experts // UP_EXPERTS, [h, ids, router_pad, *weights],
        [whole((rows, depth)), pl.BlockSpec((1, 2, rows, 128), lambda e: (item, 0, 0, 0)), whole((depth, pad))] + [weight] * 4,
        [jax.ShapeDtypeStruct((rows, 4 * pad), jnp.float32)], [whole((rows, 4 * pad))], [], sends,
        rows * depth * 2 * pad * experts * 2, item)
    return outs[0], got


def act_kernel(ff, pad, uv_ref, a_ref, b_ref, out_ref):
    lane = lax.broadcasted_iota(jnp.int32, (uv_ref.shape[0], pad), 1)
    gate_a = uv_ref[:, 0:pad]
    pick = lambda ids: jnp.sum(jnp.where(lane == wide(ids, pad) + ff, gate_a, 0.0), axis=1, keepdims=True)
    log_a, log_b = pick(a_ref[...]), pick(b_ref[...])
    top = jnp.maximum(log_a, log_b)
    exp_a, exp_b = jnp.exp(log_a - top), jnp.exp(log_b - top)
    total = exp_a + exp_b

    def parts(prob):
        high = prob.astype(jnp.bfloat16).astype(jnp.float32)
        mid = (prob - high).astype(jnp.bfloat16).astype(jnp.float32)
        return high, mid, prob - high - mid

    def swiglu(gate, up):
        return gate * jax.nn.sigmoid(gate) * up

    def assemble(act, prob):
        blk = jnp.where(lane < ff, act, 0.0)
        for num, part in enumerate(parts(prob)):
            blk = jnp.where(lane == ff + num, part, blk)
        return blk.astype(jnp.bfloat16)

    out_ref[:, 0:pad] = assemble(swiglu(gate_a, uv_ref[:, pad:2 * pad]), exp_a / total)
    out_ref[:, pad:2 * pad] = assemble(swiglu(uv_ref[:, 2 * pad:3 * pad], uv_ref[:, 3 * pad:4 * pad]), exp_b / total)


def act_call(uv, ids_a, ids_b, ff, pad):
    rows = uv.shape[0]
    return pl.pallas_call(
        lambda *refs: act_kernel(ff, pad, *refs),
        out_shape=jax.ShapeDtypeStruct((rows, 2 * pad), jnp.bfloat16),
        compiler_params=pltpu.CompilerParams(vmem_limit_bytes=16 * 1024 * 1024),
        cost_estimate=pl.CostEstimate(flops=rows * pad * 600, bytes_accessed=rows * pad * 20, transcendentals=rows * pad * 2),
        name="swiglu_and_weights",
    )(uv, ids_a, ids_b)


def down_call(layer, item, m_all, ids, weights, pad, owners, quarters, sends):
    rows = m_all.shape[0]
    _, experts, ff, half = weights[0].shape
    cols = CORES * half
    tile = min(rows, 512)

    def body(m_ref, ids_ref, down_own, down_peer, out_ref, acc_ref, wide_ref, prob_ref):
        expert = pl.program_id(0)
        me_core = lax.rem(lax.axis_index('fsdp'), CORES)

        @pl.when(expert == 0)
        def _():
            @pl.loop(0, rows, step=128)
            def _(start):
                sl = pl.ds(pl.multiple_of(start, 128), 128)
                lane = lax.broadcasted_iota(jnp.int32, (128, pad), 1)
                is_prob = (lane >= ff) & (lane < ff + 3)
                for num in range(2):
                    blk = m_ref[sl, num * pad:(num + 1) * pad].astype(jnp.float32)
                    wide_ref[sl, num * pad:(num + 1) * pad] = blk
                    prob = jnp.sum(jnp.where(is_prob, blk, 0.0), axis=1, keepdims=True)
                    prob_ref[sl, num * 128:(num + 1) * 128] = jnp.broadcast_to(prob, (128, 128))
                acc_ref[sl, :] = jnp.zeros((128, cols), jnp.float32)

        for start in range(0, rows, tile):
            sl = slice(start, start + tile)
            ids_a, ids_b = ids_ref[0, 0, sl, :], ids_ref[0, 1, sl, :]
            acts, probs = [], []
            for turn in range(DOWN_EXPERTS):
                chosen = pl.program_id(0) * DOWN_EXPERTS + turn
                is_a, is_b = wide(ids_a, pad)[:, :ff] == chosen, wide(ids_b, pad)[:, :ff] == chosen
                acts.append(jnp.where(is_a, wide_ref[sl, 0:ff], jnp.where(is_b, wide_ref[sl, pad:pad + ff], 0.0)).astype(jnp.bfloat16))
                probs.append(jnp.where(ids_a == chosen, prob_ref[sl, 0:128], jnp.where(ids_b == chosen, prob_ref[sl, 128:256], 0.0)))
            for core, w_ref in ((me_core, down_own), (1 - me_core, down_peer)):
                gain = 0.0
                for turn in range(DOWN_EXPERTS):
                    prod = jnp.dot(acts[turn], w_ref[0, turn], preferred_element_type=jnp.float32)
                    gain = gain + wide(probs[turn], half) * prod
                acc_ref[sl, pl.ds(pl.multiple_of(core * half, half), half)] += gain

        @pl.when(expert == experts // DOWN_EXPERTS - 1)
        def _():
            per = rows // owners
            sub = per // quarters
            @pl.loop(0, owners * quarters)
            def _(num):
                owner, quarter = num // quarters, num % quarters
                to = pl.ds(pl.multiple_of(owner * sub, sub), sub)
                out_ref[quarter, to, :] = acc_ref[pl.ds(pl.multiple_of(num * sub, sub), sub), :].astype(jnp.bfloat16)

    whole = lambda shape: pl.BlockSpec(shape, lambda e: (0,) * len(shape))
    weight = pl.BlockSpec((1, DOWN_EXPERTS, ff, half), lambda e: (layer, e, 0, 0))
    out_shape = (quarters, rows // quarters, cols)
    outs, got = carry(
        "down", body, experts // DOWN_EXPERTS, [m_all, ids, *weights],
        [whole((rows, 2 * pad)), pl.BlockSpec((1, 2, rows, 128), lambda e: (item, 0, 0, 0)), weight, weight],
        [jax.ShapeDtypeStruct(out_shape, jnp.bfloat16)], [whole(out_shape)],
        [pltpu.VMEM((rows, cols), jnp.float32), pltpu.VMEM((rows, 2 * pad), jnp.float32), pltpu.VMEM((rows, 256), jnp.float32)], sends,
        rows * pad * cols * experts * 2, item)
    return outs[0], got


def send_only(sends):
    return carry("move", None, 1, [], [], [], [], [], sends, 1 << 30)[1]


def solution(mesh):
    tok_axes = ('dp', 'fsdp')
    quarters = mesh.shape['tp']
    owners = mesh.shape['fsdp'] // CORES
    lines = [[chip * CORES + core for chip in range(owners)] for core in range(CORES)]
    swap = [(src, src // CORES * CORES + (src + 1) % CORES) for src in range(mesh.shape['fsdp'])]

    def exchange_x(part):
        blocks = jnp.broadcast_to(part[None], (owners,) + part.shape)
        return lax.all_to_all(blocks, 'fsdp', split_axis=0, concat_axis=0, tiled=True, axis_index_groups=lines)

    def local_step(hidden, routes, norm_gain, router, w_gate, w_up, w_down):
        layers, num_tokens, _ = routes.shape
        dim = hidden.shape[1]
        half, ff, experts = w_gate.shape[2], w_gate.shape[3], w_gate.shape[1]
        block = half * CORES
        pad = -(-(ff + experts) // 128) * 128
        per = num_tokens // CHUNKS
        sub = per // quarters
        me_chip, me_t = lax.axis_index('fsdp') // CORES, lax.axis_index('tp')
        total = layers * CHUNKS

        def tokens(item):
            return slice(item % CHUNKS * per, (item % CHUNKS + 1) * per)

        def lanes(ids):
            return jnp.broadcast_to(ids.reshape(-1)[:, None], (ids.size, 128))

        def send_input(chunk):
            rows = pl.ds(chunk * per, per)
            return Send("x%d" % chunk, 'fsdp', owners, hidden, (owners, per, block), (per, block),
                        lambda ref, peer: ref.at[rows, pl.ds(pl.multiple_of(peer * block, block), block)], lambda ref, me: ref.at[me])

        def send_part(chunk):
            return Send("part%d" % chunk, 'fsdp', owners, hidden, (owners, sub, block), (sub, block),
                        lambda ref, peer: ref.at[pl.ds(pl.multiple_of(chunk * per + lax.axis_index('tp') * sub, sub), sub), pl.ds(pl.multiple_of(peer * block, block), block)], lambda ref, me: ref.at[me])

        def send_squares(item, part):
            return Send("squares%d" % item, 'fsdp', owners, part, (owners,) + part.shape, part.shape, lambda ref, peer: ref, lambda ref, me: ref.at[me])

        def send_act(act):
            return Send("act", 'fsdp', owners, act, (owners,) + act.shape, act.shape, lambda ref, peer: ref, lambda ref, me: ref.at[me], lambda ref, at, num: ref.at[at, pl.ds(num * (per // 2), per // 2)])

        def send_sum(y):
            return Send("sum", 'tp', quarters, y, y.shape, y.shape[1:], lambda ref, peer: ref.at[peer], lambda ref, me: ref.at[me])

        def send_h(h):
            return Send("h", 'tp', quarters, h, (owners, quarters) + h.shape[1:], h.shape, lambda ref, peer: ref, lambda ref, me: ref.at[:, me], lambda ref, at, num: ref.at[pl.ds(num * (owners // 2), owners // 2), at])

        def send_rows(x):
            return Send("rows", 'fsdp', owners, x, (sub, dim), (sub, block), lambda ref, peer: ref.at[peer],
                        lambda ref, me: ref.at[:, pl.ds(pl.multiple_of(me * block, block), block)])

        def send_out(x):
            return Send("out", 'tp', quarters, x, (quarters,) + x.shape, x.shape, lambda ref, peer: ref, lambda ref, me: ref.at[me], lambda ref, at, num: ref.at[at, pl.ds(num * (sub // 2), sub // 2)])

        hidden_f = hidden.astype(jnp.float32)
        inv_own = lax.rsqrt(jnp.mean(hidden_f * hidden_f, axis=-1) + NORM_EPS)
        facts = jnp.concatenate([inv_own[None], routes.transpose(0, 2, 1).reshape(-1, num_tokens).astype(jnp.float32)], axis=0)
        facts = exchange_x(facts)
        inv_all = facts[:, 0]
        all_routes = facts[:, 1:].astype(jnp.int32).reshape(owners, layers, 2, num_tokens)

        def pair(weight):
            return weight, lax.ppermute(weight, 'fsdp', swap)

        up_weights = pair(w_gate.swapaxes(2, 3)) + pair(w_up.swapaxes(2, 3))
        down_weights = pair(w_down)
        gains = lax.dynamic_slice_in_dim(norm_gain, me_chip * block, block, 1).astype(jnp.float32)
        my_router = lax.dynamic_slice_in_dim(router, me_chip * block, block, 1)
        router_pad = jnp.pad(my_router, ((0, 0), (0, 0), (ff, pad - ff - experts)))
        ids = all_routes.reshape(owners, layers, 2, CHUNKS, per).transpose(1, 3, 2, 0, 4).reshape(total, 2, owners * per, 1)
        ids = jnp.broadcast_to(ids, ids.shape[:3] + (128,))
        own = [[lanes(routes[item // CHUNKS, tokens(item), num]) for num in range(2)] for item in range(total)]

        h, x_quarter, uv, act, m_all, y, ready, rows, out = {}, {}, {}, {}, {}, {}, {}, {}, {}

        def arrive_input(chunk, x_all):
            x_f = x_all.astype(jnp.float32)
            h[chunk] = (x_f * inv_all[:, tokens(chunk), None] * gains[0]).astype(jnp.bfloat16).reshape(owners * per, block)
            x_quarter[chunk] = lax.dynamic_slice_in_dim(x_all, me_t * sub, sub, 1)

        def arrive_part(chunk, got):
            x_quarter[chunk] = got
            inv = lax.dynamic_slice_in_dim(inv_all, chunk * per + me_t * sub, sub, 1)
            ready[chunk - CHUNKS] = (got.astype(jnp.float32) * inv[:, :, None] * gains[0]).astype(jnp.bfloat16)

        def arrive_act(item, got):
            m_all[item] = got.reshape(owners * per, 2 * pad)

        def arrive_sum(item, got):
            summed = jnp.sum(got.astype(jnp.float32), axis=0).reshape(owners, sub, block)
            x_new = (x_quarter[item].astype(jnp.float32) + summed).astype(jnp.bfloat16)
            ready[item] = x_new
            if item + CHUNKS < total:
                x_f = x_new.astype(jnp.float32)
                squares = jnp.sum(send_only([send_squares(item, jnp.sum(x_f * x_f, axis=-1))])[0], axis=0)
                inv = lax.rsqrt(squares / dim + NORM_EPS)
                x_quarter[item + CHUNKS] = x_new
                ready[item] = (x_f * inv[:, :, None] * gains[item // CHUNKS + 1]).astype(jnp.bfloat16)

        def arrive_h(item, got):
            h[item + CHUNKS] = got.reshape(owners * per, block)

        def arrive_rows(item, got):
            rows[item] = got

        def arrive_out(item, got):
            out[item] = got.reshape(per, dim)

        def inner(item):
            return item + CHUNKS < total

        first = [send_input(0)] + [send_part(chunk) for chunk in range(1, 2)]
        got = send_only(first)
        arrive_input(0, got[0])
        arrive_part(1, got[1])
        for step in range(total + 4):
            work = []
            if step == 0:
                for chunk in range(2, CHUNKS):
                    work.append((send_part(chunk), arrive_part, chunk))
            if step + 1 < CHUNKS:
                work.append((send_h(ready[step + 1 - CHUNKS]), arrive_h, step + 1 - CHUNKS))
            if 0 <= step - 2 < total:
                item = step - 2
                uv_own = lax.psum_scatter(uv[item], 'fsdp', scatter_dimension=0, tiled=True, axis_index_groups=lines)
                act[item] = act_call(uv_own, own[item][0], own[item][1], ff, pad)
                work.append((send_act(act[item]), arrive_act, item))
            if 0 <= step - 3 < total:
                work.append((send_sum(y[step - 3]), arrive_sum, step - 3))
            sends = [entry[0] for entry in work]
            if step < total:
                uv[step], got = up_call(step // CHUNKS, step, h[step], ids, router_pad[step // CHUNKS], up_weights, sends)
            else:
                got = send_only(sends) if sends else []
            for (_, arrive, item), value in zip(work, got):
                arrive(item, value)
            work = []
            if 0 <= step - 4 < total and not inner(step - 4):
                work.append((send_out(rows[step - 4]), arrive_out, step - 4))
            if 0 <= step - 3 < total:
                if inner(step - 3):
                    work.append((send_h(ready[step - 3]), arrive_h, step - 3))
                else:
                    work.append((send_rows(ready[step - 3]), arrive_rows, step - 3))
            sends = [entry[0] for entry in work]
            got = []
            if 0 <= step - 2 < total:
                item = step - 2
                y[item], got = down_call(item // CHUNKS, item, m_all[item], ids, down_weights, pad, owners, quarters, sends)
            elif sends:
                got = send_only(sends)
            for (_, arrive, item), value in zip(work, got):
                arrive(item, value)
        return jnp.concatenate([out[item] for item in range(total - CHUNKS, total)], axis=0)

    weight_in = P(None, None, 'fsdp', 'tp')
    weight_out = P(None, None, 'tp', 'fsdp')
    return jax.shard_map(local_step, mesh=mesh, in_specs=(P(tok_axes, None), P(None, tok_axes, None), P(None, None), P(None, None, None), weight_in, weight_in, weight_out), out_specs=P(tok_axes, None), check_vma=False)
```
